32 devices in a mesh: expert: 4 (over y, core), shard: 8 (over z, x).
Axes of the slice: x: 2, y: 2, z: 4, core: 2. Of those that a mesh axis runs over, the one named last changes fastest.
Arguments:
- master_down: float32 [16, 6400, 4096], P('expert', None, 'shard'), may hold values from -0.109375 to 0.109375
- second_down: bfloat16 [16, 6400, 4096], P('expert', None, 'shard'), may hold values from -0.0390625 to 0.0390625
- router_weight: float32 [4096, 16], P('shard', 'expert'), may hold values from -0.09375 to 0.09375
- router_gain: float32 [4096], P('shard'), may hold values from 0.25 to 1.75
Outputs:
- final_down: bfloat16 [16, 6400, 4096], P('expert', 'shard')
- scale_down: float32 [16, 6400], P('expert', 'shard')
- serve_router: bfloat16 [4096, 16], replicated
The draws below stay inside these ranges and needn't reach their ends.
All inputs are finite; a program needn't handle non-finite values.
Results may differ from the reference program's by a relative error of at most 0.0085.
Values may be sent and summed in bfloat16 or wider, within the bound.
A program may use at most 256 MiB of HBM per device.

```python
import jax
import jax.numpy as jnp
from jax import lax

EXPERTS = 16
D_MODEL = 4096
D_EXPERT = 6400


def strengthened(values, own_key, source, target, shards_of, factor):
    def block_of(position):
        return (jnp.arange(values.shape[position]) // (values.shape[position] // shards_of)).reshape((-1,) + (1,) * (values.ndim - 1 - position))

    one_side = jax.random.permutation(own_key, shards_of)[block_of(target)]
    other_side = (block_of(target) + shards_of // 2) % shards_of
    return jnp.where((block_of(source) == one_side) | (block_of(source) == other_side), factor * values, values)


def steps_of(rng, dims, pieces, low, high):
    gain, own = 1.0, jax.random.fold_in(rng, 6)
    for axis_at, parts in pieces:
        steps = jnp.exp(jax.random.uniform(jax.random.fold_in(own, axis_at), (parts,), jnp.float32, low / len(pieces), high / len(pieces)))
        gain = gain * jnp.repeat(steps, dims[axis_at] // parts).reshape([-1 if axis == axis_at else 1 for axis in range(len(dims))])
    return gain


def gaussian(own_key, shape, scale, reach, cuts=(), held_as=jnp.bfloat16):
    level = steps_of(own_key, shape, cuts, -0.22, 0.18) if cuts else 1.0
    values = jax.random.normal(own_key, shape, jnp.float32) * scale * level
    return jnp.minimum(jnp.maximum(values, -reach), reach).astype(held_as)


def bell_draw_with(stream_key, shape, deviation, most, cuts, heavy, held_as=jnp.bfloat16):
    drawn = deviation * jax.random.normal(stream_key, shape, jnp.float32)
    if cuts:
        drawn = drawn * steps_of(stream_key, shape, cuts, -0.22, 0.18)
    return jnp.clip(strengthened(drawn, jax.random.fold_in(stream_key, 3), *heavy), -most, most).astype(held_as)


def setup_inputs(seed: int = 0) -> dict:
    key_list = jax.random.split(jax.random.key(seed), 5)
    master_down = bell_draw_with(key_list[0], (EXPERTS, D_EXPERT, D_MODEL), D_EXPERT ** -0.5, 0.109375, ((0, 4), (2, 8)), (2, 1, 8, 2.0), jnp.float32)
    second_down = gaussian(key_list[1], (EXPERTS, D_EXPERT, D_MODEL), (D_EXPERT * 4) ** -0.5, 0.0390625, ((0, 4), (2, 8)))
    router_weight = gaussian(key_list[2], (D_MODEL, EXPERTS), D_MODEL ** -0.5, 0.09375, ((0, 8), (1, 4)), jnp.float32)
    router_gain = jnp.clip(1.0 + 0.15 * jax.random.normal(key_list[3], (D_MODEL,), jnp.float32), 0.25, 1.75)
    return {"master_down": master_down, "second_down": second_down, "router_weight": router_weight, "router_gain": router_gain}


def reference(master_down, second_down, router_weight, router_gain):
    merged_down = master_down + second_down.astype(jnp.float32)
    scale_down = jnp.sqrt(lax.optimization_barrier(jnp.sum(merged_down * merged_down, axis=2)))
    final_down = (merged_down / jnp.expand_dims(scale_down, 2)).astype(jnp.bfloat16)
    serve_router = (router_weight * router_gain[:, None]).astype(jnp.bfloat16)
    return (final_down, scale_down, serve_router)
```

```python
import functools

import jax
import jax.numpy as jnp
from jax import lax
from jax.experimental import pallas as pl
from jax.experimental.pallas import tpu as pltpu
from jax.sharding import PartitionSpec as P

ANY = pl.BlockSpec(memory_space=pl.ANY)
MESH = pl.DeviceIdType.MESH


def rows_of(rows, most):
    best = [r for r in range(8, min(rows, most) + 1, 8) if rows % r == 0]
    return best[-1] if best else rows


def merge(master_ref, second_ref, out_ref):
    out_ref[...] = (master_ref[...] + second_ref[...].astype(jnp.float32)).astype(out_ref.dtype)


def exchange(shards, experts, held, order, step_rows, master, second, router, got, staged, routers,
             send_sem, recv_sem, rsend_sem, rrecv_sem, esend_sem, erecv_sem, own_sem):
    me = lax.axis_index("shard")
    mine = lax.axis_index("expert")
    rows, columns = got.shape[2:]

    barrier = pltpu.get_barrier_semaphore()

    def greet_shard(k, carry):
        pl.semaphore_signal(barrier, inc=1, device_id={"shard": lax.rem(me + k, shards)}, device_id_type=MESH)
        return carry

    def greet_expert(k, carry):
        pl.semaphore_signal(barrier, inc=1, device_id={"expert": lax.rem(mine + k, experts)}, device_id_type=MESH)
        return carry

    lax.fori_loop(1, shards, greet_shard, 0)
    lax.fori_loop(1, experts, greet_expert, 0)
    pl.semaphore_wait(barrier, shards + experts - 2)

    def router_rows(to, origin):
        return pltpu.make_async_remote_copy(
            src_ref=router, dst_ref=routers.at[mine, me], send_sem=rsend_sem.at[to], recv_sem=rrecv_sem.at[origin],
            device_id={"shard": to}, device_id_type=MESH)

    def router_columns(to, origin):
        return pltpu.make_async_remote_copy(
            src_ref=routers.at[mine], dst_ref=routers.at[mine], send_sem=esend_sem.at[to], recv_sem=erecv_sem.at[origin],
            device_id={"expert": to}, device_id_type=MESH)

    def block(to, origin, e):
        return pltpu.make_async_remote_copy(
            src_ref=staged.at[to, e], dst_ref=got.at[me, e], send_sem=send_sem.at[to, e], recv_sem=recv_sem.at[origin, e],
            device_id={"shard": to}, device_id_type=MESH)

    own_router = pltpu.make_async_copy(router, routers.at[mine, me], own_sem)
    own_router.start()

    def start_rows(k, carry):
        router_rows(lax.rem(me + k, shards), me).start()
        return carry

    lax.fori_loop(1, shards, start_rows, 0)

    spec = pl.BlockSpec((step_rows, columns), lambda i: (i, 0))
    merged = pltpu.emit_pipeline(merge, grid=(rows // step_rows,), in_specs=[spec, spec], out_specs=[spec])

    def send_block(i, carry):
        e, k = i // (shards - 1), lax.rem(i, shards - 1)
        to = lax.rem(me + order(k, mine, e), shards)
        merged(master.at[e, to], second.at[e, to], staged.at[to, e])
        block(to, me, e).start()
        return carry

    lax.fori_loop(0, held * (shards - 1), send_block, 0)

    def wait_rows(k, carry):
        peer = lax.rem(me + k, shards)
        router_rows(peer, peer).wait()
        return carry

    own_router.wait()
    lax.fori_loop(1, shards, wait_rows, 0)

    def start_columns(k, carry):
        router_columns(lax.rem(mine + k, experts), mine).start()
        return carry

    lax.fori_loop(1, experts, start_columns, 0)

    def own_block(e, carry):
        merged(master.at[e, me], second.at[e, me], got.at[me, e])
        return carry

    lax.fori_loop(0, held, own_block, 0)

    def wait_columns(k, carry):
        peer = lax.rem(mine + k, experts)
        router_columns(peer, peer).wait()
        return carry

    lax.fori_loop(1, experts, wait_columns, 0)

    def wait_block(i, carry):
        e, k = i // (shards - 1), lax.rem(i, shards - 1)
        peer = lax.rem(me + 1 + k, shards)
        block(peer, peer, e).wait()
        return carry

    lax.fori_loop(0, held * (shards - 1), wait_block, 0)


def normalise(got_ref, out_ref, scale_ref):
    shards, _, rows, columns = got_ref.shape
    total = jnp.zeros((rows, columns), jnp.float32)
    for s in range(shards):
        part = got_ref[s, 0].astype(jnp.float32)
        total = total + part * part
    scale = jnp.sqrt(jnp.sum(total, axis=1, keepdims=True))
    scale_ref[0] = scale
    inverse = 1.0 / scale
    for s in range(shards):
        out_ref[0, :, s * columns:(s + 1) * columns] = (
            got_ref[s, 0].astype(jnp.float32) * inverse).astype(out_ref.dtype)


def in_turn(shards, k, mine, e):
    return 1 + k


def make(mesh, order=None, most=160, norm_rows=160):
    shards, experts = mesh.shape["shard"], mesh.shape["expert"]
    order = functools.partial(in_turn if order is None else order, shards)

    def body(master_down, second_down, router_weight, router_gain):
        held, wide, columns = master_down.shape
        rows = wide // shards
        router = (router_weight * router_gain[:, None]).astype(jnp.bfloat16).T
        step_rows = rows_of(rows, most)
        got, _, routers = pl.pallas_call(
            functools.partial(exchange, shards, experts, held, order, step_rows),
            out_shape=[
                jax.ShapeDtypeStruct((shards, held, rows, columns), jnp.bfloat16),
                jax.ShapeDtypeStruct((shards, held, rows, columns), jnp.bfloat16),
                jax.ShapeDtypeStruct((experts, shards) + router.shape, jnp.bfloat16),
            ],
            in_specs=[ANY] * 3,
            out_specs=[ANY] * 3,
            scratch_shapes=[
                pltpu.SemaphoreType.DMA((shards, held)),
                pltpu.SemaphoreType.DMA((shards, held)),
                pltpu.SemaphoreType.DMA((shards,)),
                pltpu.SemaphoreType.DMA((shards,)),
                pltpu.SemaphoreType.DMA((experts,)),
                pltpu.SemaphoreType.DMA((experts,)),
                pltpu.SemaphoreType.DMA,
            ],
            compiler_params=pltpu.CompilerParams(collective_id=0, has_side_effects=True),
            name="exchange",
        )(
            master_down.reshape(held, shards, rows, columns),
            second_down.reshape(held, shards, rows, columns),
            router,
        )
        norm = rows_of(rows, norm_rows)
        final_down, scale_down = pl.pallas_call(
            normalise,
            grid=(held, rows // norm),
            in_specs=[pl.BlockSpec((shards, 1, norm, columns), lambda e, i: (0, e, i, 0))],
            out_specs=[
                pl.BlockSpec((1, norm, shards * columns), lambda e, i: (e, i, 0)),
                pl.BlockSpec((1, norm, 1), lambda e, i: (e, i, 0)),
            ],
            out_shape=[
                jax.ShapeDtypeStruct((held, rows, shards * columns), jnp.bfloat16),
                jax.ShapeDtypeStruct((held, rows, 1), jnp.float32),
            ],
            name="normalise",
        )(got)
        serve_router = routers.transpose(1, 3, 0, 2).reshape(shards * router.shape[1], experts * router.shape[0])
        return final_down, scale_down[:, :, 0], serve_router

    placed = (P("expert", None, "shard"), P("expert", None, "shard"), P("shard", "expert"), P("shard"))
    return jax.shard_map(
        body,
        mesh=mesh,
        in_specs=placed,
        out_specs=(P("expert", "shard", None), P("expert", "shard"), P()),
        check_vma=False,
    )


def solution(mesh):
    return make(mesh)
```
